32 devices in a mesh: pair: 4 (over x, core), dp: 8 (over z, y).
Axes of the slice: x: 2, y: 2, z: 4, core: 2. Of those that a mesh axis runs over, the one named last changes fastest.
Arguments:
- master: float32 [4, 131072], P('pair', 'dp'), may hold values from -6 to 6
- moment1: float32 [4, 131072], P('pair', 'dp'), may hold values from -4 to 4
- moment2: float32 [4, 131072], P('pair', 'dp'), may hold values from 0.05 to 2
- local_grad: bfloat16 [4, 8, 131072], P('pair', 'dp'), may hold values from -6 to 6
- partner: int32 [8, 4], P('dp'), may hold values from 0 to 3, as said below
Outputs:
- new_master: float32 [4, 8, 2, 16384], P('pair', 'dp')
- new_moment1: float32 [4, 8, 2, 16384], P('pair', 'dp')
- new_moment2: float32 [4, 8, 2, 16384], P('pair', 'dp')
The draws below stay inside these ranges and needn't reach their ends.
Inputs may be any that keep to these rules, and one draw needn't show every extreme that they name: partner[d, partner[d, i]] == i and partner[d, i] != i for every d and i: each row a perfect matching of the 4 pair indices.
All inputs are finite; a program needn't handle non-finite values.
Results may differ from the reference program's by a relative error of at most 0.0003.
Values sent between devices are 32-bit elements; how exact they have to be, the bound alone decides.
A program may use at most 64 MiB of HBM per device.

```python
import math
import jax
import jax.numpy as jnp
from jax import lax

SH = 16384
NSH = 131072
N_PAIR = 4
N_DP = 8


def draw_partner(key, part):
    xor_masks = jax.random.randint(key, (N_DP, 1), 1, 4, dtype=jnp.int32)
    return jnp.bitwise_xor(jnp.arange(N_PAIR, dtype=jnp.int32)[None, :], xor_masks)


def with_spikes(entries, own_key, source, target, shards_of, factor):
    owner, partner = [(jnp.arange(entries.shape[dim]) // (entries.shape[dim] // shards_of)).reshape([-1 if axis == dim else 1 for axis in range(entries.ndim)]) for dim in (source, target)]
    chosen = jax.random.permutation(own_key, shards_of)[partner]
    strong = (owner == chosen) | (owner == (partner + shards_of // 2) % shards_of)
    return jnp.where(strong, factor * entries, entries)


def shard_levels(rng, dims, cuts, least, largest):
    def one(axis_at, shards_of):
        draws = jax.random.uniform(jax.random.fold_in(jax.random.fold_in(rng, 6), axis_at), (shards_of,), jnp.float32, least / len(cuts), largest / len(cuts))
        return jnp.repeat(jnp.exp(draws), dims[axis_at] // shards_of).reshape((-1,) + (1,) * (len(dims) - axis_at - 1))

    loudness = one(*cuts[0])
    for cut in cuts[1:]:
        loudness = loudness * one(*cut)
    return loudness


def scatter_about(rng, dims, scale, reach, split=(), kind=jnp.bfloat16):
    result = jax.random.normal(rng, dims, jnp.float32) * scale
    if len(split) > 0:
        result = shard_levels(rng, dims, split, -0.22, 0.18) * result
    return jnp.clip(result, min=-reach, max=reach).astype(kind)


def noise_with(stream_key, shape, deviation, most, shards, heavy, held_as=jnp.bfloat16):
    entries = deviation * jax.random.normal(stream_key, shape, jnp.float32)
    if shards:
        entries = entries * shard_levels(stream_key, shape, shards, -0.22, 0.18)
    return jnp.clip(with_spikes(entries, jax.random.fold_in(stream_key, 3), *heavy), -most, most).astype(held_as)


def setup_inputs(seed: int = 0) -> dict:
    streams_of = jax.random.split(jax.random.key(seed), 6)
    master = scatter_about(streams_of[0], (N_PAIR, NSH), 1.0, 6.0, ((0, 4), (1, 8)), jnp.float32)
    moment1 = scatter_about(streams_of[1], (N_PAIR, NSH), 0.5, 4.0, ((0, 4), (1, 8)), jnp.float32)
    moment2 = jnp.clip(jnp.exp(math.log(2.0) - 3.6888794 * jax.random.uniform(streams_of[2], (N_PAIR, NSH), jnp.float32) ** shard_levels(streams_of[2], (N_PAIR, NSH), ((0, 4), (1, 8)), -0.2, 0.2)), 0.05, 2.0)
    local_grad = noise_with(streams_of[3], (N_PAIR, N_DP, NSH), 1.0, 6.0, ((0, 4), (1, 8)), (1, 2, 8, 2.0))
    partner = draw_partner(jax.random.fold_in(streams_of[5], 71), 0)
    return dict(master=master, moment1=moment1, moment2=moment2, local_grad=local_grad, partner=partner)


beta_one = 0.9
beta_two = 0.95
bias_one = 1.0 - 0.9 ** 10
bias_two = 1.0 - 0.95 ** 10
rate = 0.001
decay = 0.1
eps_value = 1e-08

def adamw_update(weights, first, second, grads, scale):
    scaled = scale * grads
    first_new = beta_one * first + (1.0 - beta_one) * scaled
    second_new = beta_two * second + (1.0 - beta_two) * scaled * scaled
    change = first_new / bias_one / (jnp.sqrt(second_new / bias_two) + eps_value) + decay * weights
    return (weights - rate * change, first_new, second_new)

def reference(master, moment1, moment2, local_grad, partner):
    n_pair = master.shape[0]
    columns = master.shape[1]

    def add_block(index, running):
        return running + lax.dynamic_index_in_dim(local_grad, index, 1, keepdims=False).astype(jnp.float32)
    total = lax.fori_loop(0, N_DP, add_block, jnp.zeros((n_pair, columns), jnp.float32))
    norm2 = jnp.sum(total * total)
    scale = 1.0 / jnp.maximum(jnp.sqrt(norm2 / (n_pair * columns)), 1.0)
    weights, first, second = adamw_update(master, moment1, moment2, total, scale)
    owners = jnp.arange(n_pair, dtype=jnp.int32)
    mates = jnp.transpose(partner).astype(jnp.int32)
    survive = owners[:, None] < mates

    def arrange(values):
        blocks = values.reshape(n_pair, N_DP, SH)
        other = jnp.take_along_axis(blocks, mates[:, :, None], axis=0)
        paired = jnp.stack([blocks, other], axis=2)
        return jnp.where(survive[:, :, None, None], paired, 0.0)
    return (arrange(weights), arrange(first), arrange(second))
```

```python
import functools

import jax
import jax.numpy as jnp
from jax import lax
from jax.experimental import pallas as pl
from jax.experimental.pallas import tpu as pltpu
from jax.sharding import PartitionSpec as P

MESH = pl.DeviceIdType.MESH
LANES = 128

beta_one = 0.9
beta_two = 0.95
bias_one = 1.0 - 0.9**10
bias_two = 1.0 - 0.95**10
rate = 0.001
decay = 0.1
eps_value = 1e-08


def adamw_update(weights, first, second, grads, scale):
    scaled = scale * grads
    first_new = beta_one * first + (1.0 - beta_one) * scaled
    second_new = beta_two * second + (1.0 - beta_two) * scaled * scaled
    change = first_new / bias_one / (jnp.sqrt(second_new / bias_two) + eps_value) + decay * weights
    return (weights - rate * change, first_new, second_new)


def near_split(n):
    inner = 1
    while n % (inner * 2) == 0 and (inner * 2) ** 2 <= n:
        inner *= 2
    return n // inner, inner


def remote(src, dst, send_sem, recv_sem, **where):
    return pltpu.make_async_remote_copy(
        src_ref=src,
        dst_ref=dst,
        send_sem=send_sem,
        recv_sem=recv_sem,
        device_id=where,
        device_id_type=MESH,
    )


def kernel(
    n_pair,
    n_dp,
    partner,
    master,
    moment1,
    moment2,
    grad,
    out_w,
    out_m,
    out_v,
    own,
    theirs,
    near,
    partial,
    far,
    total,
    theirs_total,
    norm_pair,
    norm_pair_in,
    norm_dp,
    norm_dp_in,
    own_sem,
    state_send,
    state_recv,
    near_send,
    near_recv,
    far_send,
    far_recv,
    total_send,
    total_recv,
    pair_send,
    pair_recv,
    dp_send,
    dp_recv,
):
    outer, inner = near_split(n_dp)
    mine = lax.axis_index("pair")
    me = lax.axis_index("dp")
    a, b = lax.div(me, inner), lax.rem(me, inner)
    rows = master.shape[0]
    order = sorted(range(1, outer), key=lambda k: abs(2 * k - outer)) + [0]

    barrier = pltpu.get_barrier_semaphore()
    for k in range(1, n_dp):
        pl.semaphore_signal(barrier, inc=1, device_id={"dp": lax.rem(me + k, n_dp)}, device_id_type=MESH)
    for k in range(1, n_pair):
        pl.semaphore_signal(barrier, inc=1, device_id={"pair": lax.rem(mine + k, n_pair)}, device_id_type=MESH)

    states = (master, moment1, moment2)
    loads = [pltpu.make_async_copy(ref, own.at[i], own_sem.at[i]) for i, ref in enumerate(states)]
    for load in loads:
        load.start()
    pl.semaphore_wait(barrier, n_dp + n_pair - 2)

    def near_copy(j, k):
        to = a * inner + lax.rem(b + j, inner)
        block = lax.rem(a + k, outer) * inner + lax.rem(b + j, inner)
        return remote(grad.at[block], near.at[j - 1, k], near_send.at[j - 1, k], near_recv.at[j - 1, k], dp=to)

    for k in order:
        for j in range(1, inner):
            near_copy(j, k).start()

    def state_copy(q, i):
        return remote(states[i], theirs.at[mine, i], state_send.at[q, i], state_recv.at[mine, i], pair=q)

    def state_arrival(s, i):
        return remote(states[i], theirs.at[s, i], state_send.at[0, i], state_recv.at[s, i], pair=s)

    for q in range(n_pair - 1):

        @pl.when(q < mine)
        def _():
            for i in range(3):
                state_copy(q, i).start()

    def far_copy(k):
        to = lax.rem(a + k, outer) * inner + b
        return remote(partial.at[k - 1], far.at[k - 1], far_send.at[k - 1], far_recv.at[k - 1], dp=to)

    def level_one(k):
        for j in range(1, inner):
            near_copy(j, k).wait_recv()
        acc = grad[lax.rem(a + k, outer) * inner + b]
        for j in range(1, inner):
            acc = acc + near[j - 1, k]
        return acc

    for k in order[:-1]:
        partial[k - 1] = level_one(k)
        far_copy(k).start()
    acc = level_one(0)
    for k in order[:-1]:
        far_copy(k).wait_recv()
        acc = acc + far[k - 1]
    total[...] = acc

    def tile_sum(x):
        return jnp.sum(x.reshape(rows // 8, 8, LANES), axis=0)

    norm_pair[...] = tile_sum(acc * acc)

    def pair_copy(k):
        to = lax.rem(mine + k, n_pair)
        return remote(norm_pair, norm_pair_in.at[k - 1], pair_send.at[k - 1], pair_recv.at[k - 1], pair=to)

    for k in range(1, n_pair):
        pair_copy(k).start()

    def total_copy(q):
        return remote(total, theirs_total.at[mine], total_send.at[q], total_recv.at[mine], pair=q)

    def total_arrival(s):
        return remote(total, theirs_total.at[s], total_send.at[0], total_recv.at[s], pair=s)

    for q in range(n_pair - 1):

        @pl.when(q < mine)
        def _():
            total_copy(q).start()

    norm = norm_pair[...]
    for k in range(1, n_pair):
        pair_copy(k).wait_recv()
        norm = norm + norm_pair_in[k - 1]
    norm_dp[...] = norm

    def dp_copy(k):
        to = lax.rem(me + k, n_dp)
        return remote(norm_dp, norm_dp_in.at[k - 1], dp_send.at[k - 1], dp_recv.at[k - 1], dp=to)

    for k in range(1, n_dp):
        dp_copy(k).start()

    for load in loads:
        load.wait()
    for s in range(1, n_pair):

        @pl.when(s > mine)
        def _():
            for i in range(3):
                state_arrival(s, i).wait_recv()
            total_arrival(s).wait_recv()

    for k in range(1, n_dp):
        dp_copy(k).wait_recv()
        norm = norm + norm_dp_in[k - 1]

    norm2 = jnp.sum(norm, keepdims=True)
    count = n_pair * n_dp * rows * LANES
    scale = 1.0 / jnp.maximum(jnp.sqrt(norm2 / count), 1.0)

    mate = partner[0, mine]
    survive = mate > mine
    outs = (out_w, out_m, out_v)
    for slot in range(2):
        if slot == 0:
            args = (own[0], own[1], own[2], total[...])
        else:
            args = (theirs[mate, 0], theirs[mate, 1], theirs[mate, 2], theirs_total[mate])
        for out, value in zip(outs, adamw_update(*args, scale)):
            out[pl.ds(slot, rows, stride=2), :] = jnp.where(survive, value, 0.0)

    for k in order:
        for j in range(1, inner):
            near_copy(j, k).wait_send()
    for k in order[:-1]:
        far_copy(k).wait_send()
    for k in range(1, n_pair):
        pair_copy(k).wait_send()
    for k in range(1, n_dp):
        dp_copy(k).wait_send()
    for q in range(n_pair - 1):

        @pl.when(q < mine)
        def _():
            for i in range(3):
                state_copy(q, i).wait_send()
            total_copy(q).wait_send()


def on_device(n_pair, n_dp, master, moment1, moment2, local_grad, partner):
    shard = master.shape[1]
    rows = shard // LANES
    outer, inner = near_split(n_dp)
    grad = local_grad.astype(jnp.float32).reshape(n_dp, rows, LANES)
    f32 = jnp.float32
    vmem, smem, hbm = pltpu.VMEM, pltpu.SMEM, pl.ANY
    dma = pltpu.SemaphoreType.DMA
    block = (rows, LANES)
    tile = (8, LANES)
    levels = max(outer - 1, 1)
    results = pl.pallas_call(
        functools.partial(kernel, n_pair, n_dp),
        out_shape=[jax.ShapeDtypeStruct((2 * rows, LANES), f32)] * 3,
        in_specs=[pl.BlockSpec(memory_space=smem)]
        + [pl.BlockSpec(memory_space=hbm)] * 3
        + [pl.BlockSpec(memory_space=vmem)],
        out_specs=[pl.BlockSpec(memory_space=vmem)] * 3,
        scratch_shapes=[
            vmem((3, *block), f32),
            vmem((n_pair, 3, *block), f32),
            vmem((max(inner - 1, 1), outer, *block), f32),
            vmem((levels, *block), f32),
            vmem((levels, *block), f32),
            vmem(block, f32),
            vmem((n_pair, *block), f32),
            vmem(tile, f32),
            vmem((n_pair - 1, *tile), f32),
            vmem(tile, f32),
            vmem((n_dp - 1, *tile), f32),
            dma((3,)),
            dma((n_pair, 3)),
            dma((n_pair, 3)),
            dma((max(inner - 1, 1), outer)),
            dma((max(inner - 1, 1), outer)),
            dma((levels,)),
            dma((levels,)),
            dma((n_pair,)),
            dma((n_pair,)),
            dma((n_pair - 1,)),
            dma((n_pair - 1,)),
            dma((n_dp - 1,)),
            dma((n_dp - 1,)),
        ],
        compiler_params=pltpu.CompilerParams(collective_id=0, has_side_effects=True),
    )(
        partner,
        master.reshape(block),
        moment1.reshape(block),
        moment2.reshape(block),
        grad,
    )
    return tuple(
        item.reshape(rows, 2, LANES).transpose(1, 0, 2).reshape(1, 1, 2, shard) for item in results
    )


def solution(mesh):
    n_pair, n_dp = mesh.shape["pair"], mesh.shape["dp"]
    return jax.shard_map(
        functools.partial(on_device, n_pair, n_dp),
        mesh=mesh,
        in_specs=(
            P("pair", "dp"),
            P("pair", "dp"),
            P("pair", "dp"),
            P("pair", "dp", None),
            P("dp", None),
        ),
        out_specs=(
            P("pair", "dp", None, None),
            P("pair", "dp", None, None),
            P("pair", "dp", None, None),
        ),
        check_vma=False,
    )
```

```python
import functools

import jax
import jax.numpy as jnp
from jax import lax
from jax.experimental import pallas as pl
from jax.experimental.pallas import tpu as pltpu
from jax.sharding import PartitionSpec as P

MESH = pl.DeviceIdType.MESH
LANES = 128
PARTS = 2

beta_one = 0.9
beta_two = 0.95
bias_one = 1.0 - 0.9**10
bias_two = 1.0 - 0.95**10
rate = 0.001
decay = 0.1
eps_value = 1e-08


def adamw_update(weights, first, second, grads, scale):
    scaled = scale * grads
    first_new = beta_one * first + (1.0 - beta_one) * scaled
    second_new = beta_two * second + (1.0 - beta_two) * scaled * scaled
    change = first_new / bias_one / (jnp.sqrt(second_new / bias_two) + eps_value) + decay * weights
    return (weights - rate * change, first_new, second_new)


def near_split(n):
    inner = 1
    while n % (inner * 2) == 0 and (inner * 2) ** 2 <= n:
        inner *= 2
    return n // inner, inner


def remote(src, dst, send_sem, recv_sem, **where):
    return pltpu.make_async_remote_copy(
        src_ref=src,
        dst_ref=dst,
        send_sem=send_sem,
        recv_sem=recv_sem,
        device_id=where,
        device_id_type=MESH,
    )


def kernel(
    n_pair,
    n_dp,
    partner,
    master,
    moment1,
    moment2,
    local_grad,
    out_w,
    out_m,
    out_v,
    raw,
    grad,
    own,
    theirs,
    near,
    partial,
    far,
    total,
    theirs_total,
    norm_dp,
    norm_in,
    own_sem,
    state_send,
    state_recv,
    near_send,
    near_recv,
    far_send,
    far_recv,
    total_send,
    total_recv,
    norm_send,
    norm_recv,
    raw_sem,
    up_sem,
    down_sem,
):
    outer, inner = near_split(n_dp)
    mine = lax.axis_index("pair")
    me = lax.axis_index("dp")
    a, b = lax.div(me, inner), lax.rem(me, inner)
    rows = master.shape[0]
    order = sorted(range(1, outer), key=lambda k: abs(2 * k - outer)) + [0]

    barrier = pltpu.get_barrier_semaphore()
    for j in range(1, inner):
        pl.semaphore_signal(barrier, inc=1, device_id={"dp": a * inner + lax.rem(b + j, inner)}, device_id_type=MESH)
    for k in range(1, n_pair):
        pl.semaphore_signal(barrier, inc=1, device_id={"pair": lax.rem(mine + k, n_pair)}, device_id_type=MESH)
    above, below = a < outer - 1, a > 0

    def tell(sems):
        @pl.when(above)
        def _():
            pl.semaphore_signal(sems[0], inc=1, device_id={"dp": me + inner}, device_id_type=MESH)

        @pl.when(below)
        def _():
            pl.semaphore_signal(sems[1], inc=1, device_id={"dp": me - inner}, device_id_type=MESH)

    tell((barrier, barrier))

    states = (master, moment1, moment2)
    loads = [pltpu.make_async_copy(ref, own.at[i], own_sem.at[i]) for i, ref in enumerate(states)]
    shard = rows * LANES

    def piece_of(k):
        first = lax.rem(a + k, outer) * inner
        return pl.ds(pl.multiple_of(first * shard, shard), inner * shard)

    pieces = [pltpu.make_async_copy(local_grad.at[0, :, piece_of(k)], raw.at[:, piece_of(k)], raw_sem.at[k]) for k in range(outer)]
    for k in order:
        pieces[k].start()
    for load in loads:
        load.start()

    def widen(k):
        pieces[k].wait()
        for i in range(inner):
            block = lax.rem(a + k, outer) * inner + i
            line = raw[:, pl.ds(pl.multiple_of(block * shard, shard), shard)]
            grad[block] = line.astype(jnp.float32).reshape(rows, LANES)

    for k in order:
        widen(k)
    pl.semaphore_wait(barrier, inner + n_pair - 2 + above.astype(jnp.int32) + below.astype(jnp.int32))

    part = rows // PARTS
    cuts = [pl.ds(h * part, part) for h in range(PARTS)]

    def near_copy(j, k, h):
        to = a * inner + lax.rem(b + j, inner)
        block = lax.rem(a + k, outer) * inner + lax.rem(b + j, inner)
        sems = near_send.at[j - 1, k, h], near_recv.at[j - 1, k, h]
        return remote(grad.at[block, cuts[h]], near.at[j - 1, k, cuts[h]], *sems, dp=to)

    steps = [(k, h) for k in order[:-1] for h in range(PARTS)]
    last = [(0, h) for h in range(PARTS)]
    for k, h in steps + last:
        for j in range(1, inner):
            near_copy(j, k, h).start()

    def state_copy(q, i):
        return remote(states[i], theirs.at[mine, i], state_send.at[q, i], state_recv.at[mine, i], pair=q)

    def state_arrival(s, i):
        return remote(states[i], theirs.at[s, i], state_send.at[0, i], state_recv.at[s, i], pair=s)

    for q in range(n_pair - 1):

        @pl.when(q < mine)
        def _():
            for i in range(3):
                state_copy(q, i).start()

    for r in range(outer - 2):
        tell((up_sem.at[r], down_sem.at[r]))

        @pl.when(below)
        def _():
            pl.semaphore_wait(up_sem.at[r], 1)

        @pl.when(above)
        def _():
            pl.semaphore_wait(down_sem.at[r], 1)

    def far_copy(k, h):
        to = lax.rem(a + k, outer) * inner + b
        sems = far_send.at[k - 1, h], far_recv.at[k - 1, h]
        return remote(partial.at[k - 1, cuts[h]], far.at[k - 1, cuts[h]], *sems, dp=to)

    def level_one(k, h):
        acc = grad[lax.rem(a + k, outer) * inner + b, cuts[h]]
        for j in range(1, inner):
            near_copy(j, k, h).wait_recv()
            acc = acc + near[j - 1, k, cuts[h]]
        return acc

    for k, h in steps:
        partial[k - 1, cuts[h]] = level_one(k, h)
        far_copy(k, h).start()
    for k, h in last:
        total[cuts[h]] = level_one(k, h)
    for k, h in steps:
        far_copy(k, h).wait_recv()
    acc = total[...]
    for k in order[:-1]:
        acc = acc + far[k - 1]
    total[...] = acc

    norm_dp[...] = jnp.sum(acc * acc, axis=0, keepdims=True)

    def norm_copy(i, k):
        n = i * n_dp + k - 1
        return remote(norm_dp, norm_in.at[pl.ds(n, 1)], norm_send, norm_recv, pair=lax.rem(mine + i, n_pair), dp=lax.rem(me + k, n_dp))

    peers = [(i, k) for k in range(n_dp) for i in range(n_pair) if i + k]
    for i, k in peers:
        norm_copy(i, k).start()

    def total_copy(q):
        return remote(total, theirs_total.at[mine], total_send.at[q], total_recv.at[mine], pair=q)

    def total_arrival(s):
        return remote(total, theirs_total.at[s], total_send.at[0], total_recv.at[s], pair=s)

    for q in range(n_pair - 1):

        @pl.when(q < mine)
        def _():
            total_copy(q).start()

    for load in loads:
        load.wait()
    for s in range(1, n_pair):

        @pl.when(s > mine)
        def _():
            for i in range(3):
                state_arrival(s, i).wait_recv()
            total_arrival(s).wait_recv()

    norm = norm_dp[...]
    pltpu.make_async_copy(norm_in, norm_in, norm_recv).wait()
    norm = norm + jnp.sum(norm_in[...], axis=0, keepdims=True)

    norm2 = jnp.sum(norm, keepdims=True)
    count = n_pair * n_dp * rows * LANES
    scale = 1.0 / jnp.maximum(jnp.sqrt(norm2 / count), 1.0)

    mate = partner[0, mine]
    survive = mate > mine
    outs = (out_w, out_m, out_v)
    for slot in range(2):
        if slot == 0:
            args = (own[0], own[1], own[2], total[...])
        else:
            args = (theirs[mate, 0], theirs[mate, 1], theirs[mate, 2], theirs_total[mate])
        for out, value in zip(outs, adamw_update(*args, scale)):
            out[pl.ds(slot, rows, stride=2), :] = jnp.where(survive, value, 0.0)

    for k, h in steps + last:
        for j in range(1, inner):
            near_copy(j, k, h).wait_send()
    for k, h in steps:
        far_copy(k, h).wait_send()
    pltpu.make_async_copy(norm_in, norm_in, norm_send).wait()
    for q in range(n_pair - 1):

        @pl.when(q < mine)
        def _():
            for i in range(3):
                state_copy(q, i).wait_send()
            total_copy(q).wait_send()


def put_out(in_w, in_m, in_v, out_w, out_m, out_v, sem):
    copies = [
        pltpu.make_async_copy(src, dst, sem.at[i])
        for i, (src, dst) in enumerate(((in_w, out_w), (in_m, out_m), (in_v, out_v)))
    ]
    for copy in copies:
        copy.start()
    for copy in copies:
        copy.wait()


def on_device(n_pair, n_dp, master, moment1, moment2, local_grad, partner):
    shard = master.shape[1]
    rows = shard // LANES
    outer, inner = near_split(n_dp)
    f32 = jnp.float32
    vmem, smem, hbm = pltpu.VMEM, pltpu.SMEM, pl.ANY
    dma = pltpu.SemaphoreType.DMA
    block = (rows, LANES)
    levels = max(outer - 1, 1)
    results = pl.pallas_call(
        functools.partial(kernel, n_pair, n_dp),
        out_shape=[vmem((2 * rows, LANES), f32)] * 3,
        in_specs=[pl.BlockSpec(memory_space=smem)]
        + [pl.BlockSpec(memory_space=hbm)] * 4,
        out_specs=[pl.BlockSpec(memory_space=vmem)] * 3,
        scratch_shapes=[
            vmem((1, n_dp * shard), jnp.bfloat16),
            vmem((n_dp, *block), f32),
            vmem((3, *block), f32),
            vmem((n_pair, 3, *block), f32),
            vmem((max(inner - 1, 1), outer, *block), f32),
            vmem((levels, *block), f32),
            vmem((levels, *block), f32),
            vmem(block, f32),
            vmem((n_pair, *block), f32),
            vmem((1, LANES), f32),
            vmem((n_pair * n_dp - 1, LANES), f32),
            dma((3,)),
            dma((n_pair, 3)),
            dma((n_pair, 3)),
            dma((max(inner - 1, 1), outer, PARTS)),
            dma((max(inner - 1, 1), outer, PARTS)),
            dma((levels, PARTS)),
            dma((levels, PARTS)),
            dma((n_pair,)),
            dma((n_pair,)),
            dma,
            dma,
            dma((outer,)),
            pltpu.SemaphoreType.REGULAR((max(outer - 2, 1),)),
            pltpu.SemaphoreType.REGULAR((max(outer - 2, 1),)),
        ],
        compiler_params=pltpu.CompilerParams(collective_id=0, has_side_effects=True),
    )(
        partner,
        master.reshape(block),
        moment1.reshape(block),
        moment2.reshape(block),
        local_grad,
    )
    results = pl.pallas_call(
        put_out,
        out_shape=[jax.ShapeDtypeStruct((2 * rows, LANES), f32)] * 3,
        in_specs=[pl.BlockSpec(memory_space=vmem)] * 3,
        out_specs=[pl.BlockSpec(memory_space=hbm)] * 3,
        scratch_shapes=[dma((3,))],
    )(*[pltpu.with_memory_space_constraint(item, pltpu.VMEM) for item in results])
    return tuple(
        item.reshape(rows, 2, LANES).transpose(1, 0, 2).reshape(1, 1, 2, shard) for item in results
    )


def solution(mesh):
    n_pair, n_dp = mesh.shape["pair"], mesh.shape["dp"]
    return jax.shard_map(
        functools.partial(on_device, n_pair, n_dp),
        mesh=mesh,
        in_specs=(
            P("pair", "dp"),
            P("pair", "dp"),
            P("pair", "dp"),
            P("pair", "dp", None),
            P("dp", None),
        ),
        out_specs=(
            P("pair", "dp", None, None),
            P("pair", "dp", None, None),
            P("pair", "dp", None, None),
        ),
        check_vma=False,
    )
```

```python
import functools

import jax
import jax.numpy as jnp
from jax import lax
from jax.experimental import pallas as pl
from jax.experimental.pallas import tpu as pltpu
from jax.sharding import PartitionSpec as P

MESH = pl.DeviceIdType.MESH
LANES = 128
PARTS = 2

beta_one = 0.9
beta_two = 0.95
bias_one = 1.0 - 0.9**10
bias_two = 1.0 - 0.95**10
rate = 0.001
decay = 0.1
eps_value = 1e-08


def adamw_update(weights, first, second, grads, scale):
    scaled = scale * grads
    first_new = beta_one * first + (1.0 - beta_one) * scaled
    second_new = beta_two * second + (1.0 - beta_two) * scaled * scaled
    change = first_new / bias_one / (jnp.sqrt(second_new / bias_two) + eps_value) + decay * weights
    return (weights - rate * change, first_new, second_new)


def near_split(n):
    inner = 1
    while n % (inner * 2) == 0 and (inner * 2) ** 2 <= n:
        inner *= 2
    return n // inner, inner


def remote(src, dst, send_sem, recv_sem, **where):
    return pltpu.make_async_remote_copy(
        src_ref=src,
        dst_ref=dst,
        send_sem=send_sem,
        recv_sem=recv_sem,
        device_id=where,
        device_id_type=MESH,
    )


def kernel(
    n_pair,
    n_dp,
    partner,
    master,
    moment1,
    moment2,
    local_grad,
    out_w,
    out_m,
    out_v,
    raw,
    grad,
    own,
    theirs,
    near,
    partial,
    far,
    total,
    theirs_total,
    norm_dp,
    norm_in,
    own_sem,
    state_send,
    state_recv,
    near_send,
    near_recv,
    far_send,
    far_recv,
    total_send,
    total_recv,
    norm_send,
    norm_recv,
    raw_sem,
    up_sem,
    down_sem,
):
    outer, inner = near_split(n_dp)
    mine = lax.axis_index("pair")
    me = lax.axis_index("dp")
    a, b = lax.div(me, inner), lax.rem(me, inner)
    rows = master.shape[0]
    order = sorted(range(1, outer), key=lambda k: (abs(2 * k - outer), -k)) + [0]

    def across(m):
        at = a
        for bit in (1 << e for e in range(outer.bit_length())):
            if m & bit:
                at = at + bit - 2 * bit * lax.rem(lax.div(a, bit), 2)
        return at


    barrier = pltpu.get_barrier_semaphore()
    for j in range(1, inner):
        pl.semaphore_signal(barrier, inc=1, device_id={"dp": a * inner + lax.rem(b + j, inner)}, device_id_type=MESH)
    for k in range(1, n_pair):
        pl.semaphore_signal(barrier, inc=1, device_id={"pair": lax.rem(mine + k, n_pair)}, device_id_type=MESH)
    above, below = a < outer - 1, a > 0

    def tell(sems):
        @pl.when(above)
        def _():
            pl.semaphore_signal(sems[0], inc=1, device_id={"dp": me + inner}, device_id_type=MESH)

        @pl.when(below)
        def _():
            pl.semaphore_signal(sems[1], inc=1, device_id={"dp": me - inner}, device_id_type=MESH)

    tell((barrier, barrier))

    states = (master, moment1, moment2)
    loads = [pltpu.make_async_copy(ref, own.at[i], own_sem.at[i]) for i, ref in enumerate(states)]
    shard = rows * LANES

    def piece_of(k):
        first = across(k) * inner
        return pl.ds(pl.multiple_of(first * shard, shard), inner * shard)

    pieces = [pltpu.make_async_copy(local_grad.at[0, :, piece_of(k)], raw.at[:, piece_of(k)], raw_sem.at[k]) for k in range(outer)]
    for k in order:
        pieces[k].start()
    for load in loads:
        load.start()

    def widen(k):
        pieces[k].wait()
        for i in range(inner):
            block = across(k) * inner + i
            line = raw[:, pl.ds(pl.multiple_of(block * shard, shard), shard)]
            grad[block] = line.astype(jnp.float32).reshape(rows, LANES)

    for k in order:
        widen(k)
    pl.semaphore_wait(barrier, inner + n_pair - 2 + above.astype(jnp.int32) + below.astype(jnp.int32))

    part = rows // PARTS
    cuts = [pl.ds(h * part, part) for h in range(PARTS)]

    def near_copy(j, k, h):
        to = a * inner + lax.rem(b + j, inner)
        block = across(k) * inner + lax.rem(b + j, inner)
        sems = near_send.at[j - 1, k, h], near_recv.at[j - 1, k, h]
        return remote(grad.at[block, cuts[h]], near.at[j - 1, k, cuts[h]], *sems, dp=to)

    steps = [(k, h) for k in order[:-1] for h in range(PARTS)]
    last = [(0, h) for h in range(PARTS)]
    for k, h in steps + last:
        for j in range(1, inner):
            near_copy(j, k, h).start()

    def state_copy(q, i):
        return remote(states[i], theirs.at[mine, i], state_send.at[q, i], state_recv.at[mine, i], pair=q)

    def state_arrival(s, i):
        return remote(states[i], theirs.at[s, i], state_send.at[0, i], state_recv.at[s, i], pair=s)

    for q in range(n_pair - 1):

        @pl.when(q < mine)
        def _():
            for i in range(3):
                state_copy(q, i).start()

    for r in range(outer - 2):
        tell((up_sem.at[r], down_sem.at[r]))

        @pl.when(below)
        def _():
            pl.semaphore_wait(up_sem.at[r], 1)

        @pl.when(above)
        def _():
            pl.semaphore_wait(down_sem.at[r], 1)

    def far_copy(k, h):
        to = across(k) * inner + b
        sems = far_send.at[k - 1, h], far_recv.at[k - 1, h]
        return remote(partial.at[k - 1, cuts[h]], far.at[k - 1, cuts[h]], *sems, dp=to)

    def level_one(k, h):
        acc = grad[across(k) * inner + b, cuts[h]]
        for j in range(1, inner):
            near_copy(j, k, h).wait_recv()
            acc = acc + near[j - 1, k, cuts[h]]
        return acc

    for k, h in steps:
        partial[k - 1, cuts[h]] = level_one(k, h)
        far_copy(k, h).start()
    for k, h in last:
        total[cuts[h]] = level_one(k, h)
    for k, h in steps:
        far_copy(k, h).wait_recv()
    acc = total[...]
    for k in order[:-1]:
        acc = acc + far[k - 1]
    total[...] = acc

    norm_dp[...] = jnp.sum(acc * acc, axis=0, keepdims=True)

    def norm_copy(i, k):
        n = i * n_dp + k - 1
        return remote(norm_dp, norm_in.at[pl.ds(n, 1)], norm_send, norm_recv, pair=lax.rem(mine + i, n_pair), dp=lax.rem(me + k, n_dp))

    peers = [(i, k) for k in range(n_dp) for i in range(n_pair) if i + k]
    for i, k in peers:
        norm_copy(i, k).start()

    def total_copy(q):
        return remote(total, theirs_total.at[mine], total_send.at[q], total_recv.at[mine], pair=q)

    def total_arrival(s):
        return remote(total, theirs_total.at[s], total_send.at[0], total_recv.at[s], pair=s)

    for q in range(n_pair - 1):

        @pl.when(q < mine)
        def _():
            total_copy(q).start()

    for load in loads:
        load.wait()
    for s in range(1, n_pair):

        @pl.when(s > mine)
        def _():
            for i in range(3):
                state_arrival(s, i).wait_recv()
            total_arrival(s).wait_recv()

    norm = norm_dp[...]
    pltpu.make_async_copy(norm_in, norm_in, norm_recv).wait()
    norm = norm + jnp.sum(norm_in[...], axis=0, keepdims=True)

    norm2 = jnp.sum(norm, keepdims=True)
    count = n_pair * n_dp * rows * LANES
    scale = 1.0 / jnp.maximum(jnp.sqrt(norm2 / count), 1.0)

    mate = partner[0, mine]
    survive = mate > mine
    outs = (out_w, out_m, out_v)
    for slot in range(2):
        if slot == 0:
            args = (own[0], own[1], own[2], total[...])
        else:
            args = (theirs[mate, 0], theirs[mate, 1], theirs[mate, 2], theirs_total[mate])
        for out, value in zip(outs, adamw_update(*args, scale)):
            out[pl.ds(slot, rows, stride=2), :] = jnp.where(survive, value, 0.0)

    for k, h in steps + last:
        for j in range(1, inner):
            near_copy(j, k, h).wait_send()
    for k, h in steps:
        far_copy(k, h).wait_send()
    pltpu.make_async_copy(norm_in, norm_in, norm_send).wait()
    for q in range(n_pair - 1):

        @pl.when(q < mine)
        def _():
            for i in range(3):
                state_copy(q, i).wait_send()
            total_copy(q).wait_send()


def put_out(in_w, in_m, in_v, out_w, out_m, out_v, sem):
    copies = [
        pltpu.make_async_copy(src, dst, sem.at[i])
        for i, (src, dst) in enumerate(((in_w, out_w), (in_m, out_m), (in_v, out_v)))
    ]
    for copy in copies:
        copy.start()
    for copy in copies:
        copy.wait()


def on_device(n_pair, n_dp, master, moment1, moment2, local_grad, partner):
    shard = master.shape[1]
    rows = shard // LANES
    outer, inner = near_split(n_dp)
    f32 = jnp.float32
    vmem, smem, hbm = pltpu.VMEM, pltpu.SMEM, pl.ANY
    dma = pltpu.SemaphoreType.DMA
    block = (rows, LANES)
    levels = max(outer - 1, 1)
    results = pl.pallas_call(
        functools.partial(kernel, n_pair, n_dp),
        out_shape=[vmem((2 * rows, LANES), f32)] * 3,
        in_specs=[pl.BlockSpec(memory_space=smem)]
        + [pl.BlockSpec(memory_space=hbm)] * 4,
        out_specs=[pl.BlockSpec(memory_space=vmem)] * 3,
        scratch_shapes=[
            vmem((1, n_dp * shard), jnp.bfloat16),
            vmem((n_dp, *block), f32),
            vmem((3, *block), f32),
            vmem((n_pair, 3, *block), f32),
            vmem((max(inner - 1, 1), outer, *block), f32),
            vmem((levels, *block), f32),
            vmem((levels, *block), f32),
            vmem(block, f32),
            vmem((n_pair, *block), f32),
            vmem((1, LANES), f32),
            vmem((n_pair * n_dp - 1, LANES), f32),
            dma((3,)),
            dma((n_pair, 3)),
            dma((n_pair, 3)),
            dma((max(inner - 1, 1), outer, PARTS)),
            dma((max(inner - 1, 1), outer, PARTS)),
            dma((levels, PARTS)),
            dma((levels, PARTS)),
            dma((n_pair,)),
            dma((n_pair,)),
            dma,
            dma,
            dma((outer,)),
            pltpu.SemaphoreType.REGULAR((max(outer - 2, 1),)),
            pltpu.SemaphoreType.REGULAR((max(outer - 2, 1),)),
        ],
        compiler_params=pltpu.CompilerParams(collective_id=0, has_side_effects=True),
    )(
        partner,
        master.reshape(block),
        moment1.reshape(block),
        moment2.reshape(block),
        local_grad,
    )
    results = pl.pallas_call(
        put_out,
        out_shape=[jax.ShapeDtypeStruct((2 * rows, LANES), f32)] * 3,
        in_specs=[pl.BlockSpec(memory_space=vmem)] * 3,
        out_specs=[pl.BlockSpec(memory_space=hbm)] * 3,
        scratch_shapes=[dma((3,))],
    )(*[pltpu.with_memory_space_constraint(item, pltpu.VMEM) for item in results])
    return tuple(
        item.reshape(rows, 2, LANES).transpose(1, 0, 2).reshape(1, 1, 2, shard) for item in results
    )


def solution(mesh):
    n_pair, n_dp = mesh.shape["pair"], mesh.shape["dp"]
    return jax.shard_map(
        functools.partial(on_device, n_pair, n_dp),
        mesh=mesh,
        in_specs=(
            P("pair", "dp"),
            P("pair", "dp"),
            P("pair", "dp"),
            P("pair", "dp", None),
            P("dp", None),
        ),
        out_specs=(
            P("pair", "dp", None, None),
            P("pair", "dp", None, None),
            P("pair", "dp", None, None),
        ),
        check_vma=False,
    )
```
